16 devices in a mesh: tp: 4 (over z, y), ep: 4 (over x, core).
Axes of the slice: x: 2, y: 2, z: 2, core: 2. Of those that a mesh axis runs over, the one named last changes fastest.
Arguments:
- hidden_in: bfloat16 [1536, 2048], P(('tp', 'ep'))
- cache0: bfloat16 [1536, 256, 576], P(('tp', 'ep'))
- cache1: bfloat16 [1536, 256, 576], P(('tp', 'ep'))
- kv_lens: int32 [1536], P(('tp', 'ep'))
- route_ids: int32 [1536, 6], P(('tp', 'ep'))
- route_wts: float32 [1536, 6], P(('tp', 'ep'))
- att0_q: bfloat16 [2048, 16, 192], replicated
- att0_uk: bfloat16 [16, 128, 512], replicated
- att0_uv: bfloat16 [16, 512, 128], replicated
- att0_o: bfloat16 [16, 128, 2048], replicated
- att1_q: bfloat16 [2048, 16, 192], replicated
- att1_uk: bfloat16 [16, 128, 512], replicated
- att1_uv: bfloat16 [16, 512, 128], replicated
- att1_o: bfloat16 [16, 128, 2048], replicated
- ffn0_gate: bfloat16 [2048, 10944], P(None, 'tp')
- ffn0_up: bfloat16 [2048, 10944], P(None, 'tp')
- ffn0_down: bfloat16 [10944, 2048], P('tp')
- ffn1_gate: bfloat16 [2048, 10944], P(None, 'tp')
- ffn1_up: bfloat16 [2048, 10944], P(None, 'tp')
- ffn1_down: bfloat16 [10944, 2048], P('tp')
- exp_gate: bfloat16 [16, 2048, 1408], P(('tp', 'ep'))
- exp_up: bfloat16 [16, 2048, 1408], P(('tp', 'ep'))
- exp_down: bfloat16 [16, 1408, 2048], P(('tp', 'ep'))
Outputs:
- output: bfloat16 [1536, 2048], P(('tp', 'ep'))
All inputs are finite; a program needn't handle non-finite values.
Results may differ from the reference program's by a relative error of at most 0.0155518.
Values are sent between devices in bfloat16 or wider.
A program may use at most 1 GiB of HBM per device.

```python
import jax
import jax.numpy as jnp
from jax import lax

HIDDEN = 2048
NUM_HEADS = 16
NOPE_DIM = 128
ROPE_DIM = 64
VALUE_DIM = 128
LATENT = 512
TOP_K = 6
FF_EXPERT = 1408
FF_DENSE = 10944
TOK_DEV = 96
KV_LEN = 256
ZERO_EXPERTS = 256
DEVICES = 16

NUM_TOKENS = TOK_DEV * DEVICES
SLOT_CAP = min(TOK_DEV, (2 * TOK_DEV * TOP_K + DEVICES - 1) // DEVICES)
ROWS_MAX = DEVICES * SLOT_CAP
NUM_HOT = max(1, DEVICES // 16)
COLD_SLOTS = (TOK_DEV * TOP_K * 3) // 5 - NUM_HOT * SLOT_CAP
SCALE = (NOPE_DIM + ROPE_DIM) ** -0.5


def draw_normal(key, shape, scale):
    return (jax.random.normal(key, shape, jnp.float32) * scale).astype(jnp.bfloat16)


def draw_routes(key):
    key_hot, key_src = jax.random.split(key)
    dev_order = jax.random.permutation(key_hot, DEVICES)
    hot_flag = jnp.zeros((DEVICES,), jnp.int32).at[dev_order[:NUM_HOT]].set(1)
    cold_devs = dev_order[NUM_HOT:]

    def one_source(src):
        src_key = jax.random.fold_in(key_src, src)
        key_pick, key_zero, key_perm = jax.random.split(src_key, 3)
        cold_pick = cold_devs[jax.random.randint(key_pick, (COLD_SLOTS,), 0, DEVICES - NUM_HOT)]
        dev_counts = jax.ops.segment_sum(jnp.ones((COLD_SLOTS,), jnp.int32), cold_pick, num_segments=DEVICES)
        dev_counts = jnp.where(hot_flag == 1, SLOT_CAP, jnp.minimum(dev_counts, SLOT_CAP))
        dev_bounds = jnp.cumsum(dev_counts)
        dest_dev = jnp.searchsorted(dev_bounds, jnp.arange(TOK_DEV * TOP_K), side='right').astype(jnp.int32)
        dest_dev = dest_dev.reshape(TOP_K, TOK_DEV).T
        zero_base = jax.random.randint(key_zero, (TOK_DEV, 1), 0, ZERO_EXPERTS)
        zero_ids = DEVICES + (jnp.arange(TOP_K)[None, :] + zero_base) % ZERO_EXPERTS
        slot_ids = jnp.where(dest_dev < DEVICES, dest_dev, zero_ids).astype(jnp.int32)
        return slot_ids[jax.random.permutation(key_perm, TOK_DEV)]

    return jax.vmap(one_source)(jnp.arange(DEVICES)).reshape(NUM_TOKENS, TOP_K)


def draw_lengths(key):
    lengths = jax.random.randint(key, (NUM_TOKENS,), KV_LEN // 8, KV_LEN + 1)
    return lengths.at[0].set(KV_LEN).astype(jnp.int32)


def setup_inputs(seed: int = 0) -> dict:
    keys = jax.random.split(jax.random.key(seed), 26)
    qk_dim = NOPE_DIM + ROPE_DIM
    uv_scale = LATENT ** -0.5 * KV_LEN ** 0.5 / 4.0
    return {
        'hidden_in': draw_normal(keys[0], (NUM_TOKENS, HIDDEN), 1.0),
        'cache0': draw_normal(keys[1], (NUM_TOKENS, KV_LEN, LATENT + ROPE_DIM), 1.0),
        'cache1': draw_normal(keys[2], (NUM_TOKENS, KV_LEN, LATENT + ROPE_DIM), 1.0),
        'kv_lens': draw_lengths(keys[3]),
        'route_ids': draw_routes(keys[4]),
        'route_wts': jax.random.uniform(keys[5], (NUM_TOKENS, TOP_K), jnp.float32, 0.5, 1.5) * (2.0 / TOP_K),
        'att0_q': draw_normal(keys[6], (HIDDEN, NUM_HEADS, qk_dim), HIDDEN ** -0.5),
        'att0_uk': draw_normal(keys[7], (NUM_HEADS, NOPE_DIM, LATENT), NOPE_DIM ** -0.5),
        'att0_uv': draw_normal(keys[8], (NUM_HEADS, LATENT, VALUE_DIM), uv_scale),
        'att0_o': draw_normal(keys[9], (NUM_HEADS, VALUE_DIM, HIDDEN), (NUM_HEADS * VALUE_DIM) ** -0.5),
        'att1_q': draw_normal(keys[10], (HIDDEN, NUM_HEADS, qk_dim), HIDDEN ** -0.5),
        'att1_uk': draw_normal(keys[11], (NUM_HEADS, NOPE_DIM, LATENT), NOPE_DIM ** -0.5),
        'att1_uv': draw_normal(keys[12], (NUM_HEADS, LATENT, VALUE_DIM), uv_scale),
        'att1_o': draw_normal(keys[13], (NUM_HEADS, VALUE_DIM, HIDDEN), (NUM_HEADS * VALUE_DIM) ** -0.5),
        'ffn0_gate': draw_normal(keys[14], (HIDDEN, FF_DENSE), HIDDEN ** -0.5),
        'ffn0_up': draw_normal(keys[15], (HIDDEN, FF_DENSE), HIDDEN ** -0.5),
        'ffn0_down': draw_normal(keys[16], (FF_DENSE, HIDDEN), FF_DENSE ** -0.5),
        'ffn1_gate': draw_normal(keys[17], (HIDDEN, FF_DENSE), HIDDEN ** -0.5),
        'ffn1_up': draw_normal(keys[18], (HIDDEN, FF_DENSE), HIDDEN ** -0.5),
        'ffn1_down': draw_normal(keys[19], (FF_DENSE, HIDDEN), FF_DENSE ** -0.5),
        'exp_gate': draw_normal(keys[20], (DEVICES, HIDDEN, FF_EXPERT), HIDDEN ** -0.5),
        'exp_up': draw_normal(keys[21], (DEVICES, HIDDEN, FF_EXPERT), HIDDEN ** -0.5),
        'exp_down': draw_normal(keys[22], (DEVICES, FF_EXPERT, HIDDEN), 2.0 * FF_EXPERT ** -0.5),
    }


def rms_norm(vec):
    vec32 = vec.astype(jnp.float32)
    return (vec32 * lax.rsqrt(jnp.mean(vec32 * vec32, axis=-1, keepdims=True) + 1e-6)).astype(jnp.bfloat16)


def rope_rotate(vals, pos):
    half_dim = vals.shape[-1] // 2
    inv_freq = 10000.0 ** (-2.0 * jnp.arange(half_dim, dtype=jnp.float32) / vals.shape[-1])
    rot_angle = pos.astype(jnp.float32)[..., None, None] * inv_freq
    cos_ang = jnp.cos(rot_angle)
    sin_ang = jnp.sin(rot_angle)
    lead_half = vals[..., :half_dim]
    tail_half = vals[..., half_dim:]
    return jnp.concatenate([lead_half * cos_ang - tail_half * sin_ang, tail_half * cos_ang + lead_half * sin_ang], axis=-1)


def swiglu(rows, w_gate, w_up, w_down):
    gate_val = jnp.dot(rows, w_gate, preferred_element_type=jnp.float32)
    up_val = jnp.dot(rows, w_up, preferred_element_type=jnp.float32)
    act_val = (jax.nn.silu(gate_val) * up_val).astype(jnp.bfloat16)
    return jnp.dot(act_val, w_down, preferred_element_type=jnp.float32)


def attention(normed, cache, kv_lens, w_q, w_uk, w_uv, w_o):
    wq32 = w_q.astype(jnp.float32)
    wuk32 = w_uk.astype(jnp.float32)
    wuv32 = w_uv.astype(jnp.float32)
    wo32 = w_o.astype(jnp.float32)

    def one_token(item):
        vec, kv_rows, length = item
        q_full = jnp.einsum('d,dhc->hc', vec.astype(jnp.float32), wq32).astype(jnp.bfloat16)
        q_rope = rope_rotate(q_full[:, NOPE_DIM:].astype(jnp.float32), length).astype(jnp.bfloat16)
        q_lat = jnp.einsum('hn,hnl->hl', q_full[:, :NOPE_DIM].astype(jnp.float32), wuk32).astype(jnp.bfloat16)
        q_cat = jnp.concatenate([q_lat, q_rope], axis=1)
        scores = jnp.dot(q_cat, kv_rows.T, preferred_element_type=jnp.float32) * SCALE
        valid = jnp.arange(KV_LEN)[None, :] < length
        probs = jax.nn.softmax(jnp.where(valid, scores, -1e30), axis=-1).astype(jnp.bfloat16)
        o_lat = jnp.dot(probs, kv_rows[:, :LATENT], preferred_element_type=jnp.float32).astype(jnp.bfloat16)
        o_val = jnp.einsum('hl,hlv->hv', o_lat.astype(jnp.float32), wuv32).astype(jnp.bfloat16)
        return jnp.einsum('hv,hvd->d', o_val.astype(jnp.float32), wo32)

    return lax.map(one_token, (normed, cache, kv_lens))


def expert_mix(normed, route_ids, route_wts, exp_gate, exp_up, exp_down):
    flat_ids = route_ids.reshape(-1)
    flat_wts = route_wts.reshape(-1)
    num_slots = flat_ids.shape[0]
    key_ids = jnp.where(flat_ids < DEVICES, flat_ids, DEVICES)
    slot_order = jnp.argsort(key_ids, stable=True)
    counts = jax.ops.segment_sum(jnp.ones_like(key_ids), key_ids, num_segments=DEVICES + 1)
    starts = jnp.cumsum(counts) - counts
    local_pos = jnp.arange(ROWS_MAX)

    def one_expert(carry, item):
        start, count, w_gate, w_up, w_down = item
        slot_idx = slot_order[jnp.minimum(start + local_pos, num_slots - 1)]
        tok_idx = slot_idx // TOP_K
        exp_out = swiglu(normed[tok_idx], w_gate, w_up, w_down).astype(jnp.bfloat16)
        slot_wt = jnp.where(local_pos < count, flat_wts[slot_idx], 0.0)
        return carry.at[tok_idx].add(slot_wt[:, None] * exp_out.astype(jnp.float32)), None

    mix_init = jnp.zeros((NUM_TOKENS, HIDDEN), jnp.float32)
    mix, _ = lax.scan(one_expert, mix_init, (starts[:DEVICES], counts[:DEVICES], exp_gate, exp_up, exp_down))
    zero_wt = jnp.sum(jnp.where(route_ids >= DEVICES, route_wts, 0.0), axis=1)
    return mix + zero_wt[:, None] * normed.astype(jnp.float32)


def reference(hidden_in, cache0, cache1, kv_lens, route_ids, route_wts, att0_q, att0_uk, att0_uv, att0_o, att1_q, att1_uk, att1_uv, att1_o, ffn0_gate, ffn0_up, ffn0_down, ffn1_gate, ffn1_up, ffn1_down, exp_gate, exp_up, exp_down):
    att_zero = attention(rms_norm(hidden_in), cache0, kv_lens, att0_q, att0_uk, att0_uv, att0_o)
    h_zero = (hidden_in.astype(jnp.float32) + att_zero).astype(jnp.bfloat16)
    u_zero = rms_norm(h_zero)
    f_zero = (h_zero.astype(jnp.float32) + swiglu(u_zero, ffn0_gate, ffn0_up, ffn0_down)).astype(jnp.bfloat16)
    att_one = attention(rms_norm(f_zero), cache1, kv_lens, att1_q, att1_uk, att1_uv, att1_o)
    h_one = (f_zero.astype(jnp.float32) + att_one).astype(jnp.bfloat16)
    mix = expert_mix(u_zero, route_ids, route_wts, exp_gate, exp_up, exp_down)
    dense_one = swiglu(rms_norm(h_one), ffn1_gate, ffn1_up, ffn1_down)
    return (h_one.astype(jnp.float32) + dense_one + mix).astype(jnp.bfloat16)
```

```python
import jax
import jax.numpy as jnp
from jax import lax
from jax.sharding import PartitionSpec as P

FLAT_AXES = ('tp', 'ep')


def rms_norm(vec):
    vec32 = vec.astype(jnp.float32)
    return (vec32 * lax.rsqrt(jnp.mean(vec32 * vec32, axis=-1, keepdims=True) + 1e-6)).astype(jnp.bfloat16)


def rope_rotate(vals, pos):
    half_dim = vals.shape[-1] // 2
    inv_freq = 10000.0 ** (-2.0 * jnp.arange(half_dim, dtype=jnp.float32) / vals.shape[-1])
    rot_angle = pos.astype(jnp.float32)[..., None, None] * inv_freq
    cos_ang = jnp.cos(rot_angle)
    sin_ang = jnp.sin(rot_angle)
    lead_half = vals[..., :half_dim]
    tail_half = vals[..., half_dim:]
    return jnp.concatenate([lead_half * cos_ang - tail_half * sin_ang, tail_half * cos_ang + lead_half * sin_ang], axis=-1)


def act_rows(rows, w_gate, w_up):
    gate_val = jnp.dot(rows, w_gate, preferred_element_type=jnp.float32)
    up_val = jnp.dot(rows, w_up, preferred_element_type=jnp.float32)
    return (jax.nn.silu(gate_val) * up_val).astype(jnp.bfloat16)


def attention(normed, cache, kv_lens, w_q, w_uk, w_uv, w_o):
    nope_dim = w_uk.shape[1]
    latent = w_uk.shape[2]
    scale = w_q.shape[2] ** -0.5
    q_full = jnp.einsum('bd,dhc->bhc', normed, w_q, preferred_element_type=jnp.float32).astype(jnp.bfloat16)
    q_rope = rope_rotate(q_full[..., nope_dim:].astype(jnp.float32), kv_lens).astype(jnp.bfloat16)
    q_lat = jnp.einsum('bhn,hnl->bhl', q_full[..., :nope_dim], w_uk, preferred_element_type=jnp.float32).astype(jnp.bfloat16)
    q_cat = jnp.concatenate([q_lat, q_rope], axis=-1)
    scores = jnp.einsum('bhc,bpc->bhp', q_cat, cache, preferred_element_type=jnp.float32) * scale
    valid = jnp.arange(cache.shape[1])[None, None, :] < kv_lens[:, None, None]
    probs = jax.nn.softmax(jnp.where(valid, scores, -1e30), axis=-1).astype(jnp.bfloat16)
    o_lat = jnp.einsum('bhp,bpl->bhl', probs, cache[:, :, :latent], preferred_element_type=jnp.float32).astype(jnp.bfloat16)
    o_val = jnp.einsum('bhl,hlv->bhv', o_lat, w_uv, preferred_element_type=jnp.float32).astype(jnp.bfloat16)
    return jnp.einsum('bhv,hvd->bd', o_val, w_o, preferred_element_type=jnp.float32)


def xor_send(vals, mask):
    return lax.ppermute(vals, FLAT_AXES, [(dev, dev ^ mask) for dev in range(16)])


def gather_tp(rows):
    return [rows] + [xor_send(rows, 4 * rel) for rel in (1, 2, 3)]


def reduce_tp(part):
    half = part.shape[-1] // 2
    lead, tail = part[..., :half], part[..., half:]
    lead_in = xor_send(lead[2:], 8)
    tail_in = xor_send(tail[1::2], 4)
    lead_sum = lead[:2] + lead_in
    tail_sum = tail[0::2] + tail_in
    lead_own = lead_sum[0] + xor_send(lead_sum[1], 4)
    tail_own = tail_sum[0] + xor_send(tail_sum[1], 8)
    return jnp.concatenate([lead_own, tail_own], axis=-1)


def ranks_of(hit):
    tok = hit.shape[-1]
    before = (jnp.arange(tok)[:, None] < jnp.arange(tok)[None, :]).astype(jnp.bfloat16)
    return jnp.dot(hit.astype(jnp.bfloat16), before, preferred_element_type=jnp.float32)


def solution(mesh):
    n_dev = mesh.shape['tp'] * mesh.shape['ep']
    rows_spec = P(FLAT_AXES, None)
    cube_spec = P(FLAT_AXES, None, None)
    whole_spec = P(None, None, None)
    col_split = P(None, 'tp')
    row_split = P('tp', None)
    in_specs = (rows_spec, cube_spec, cube_spec, P(FLAT_AXES), rows_spec, rows_spec,
                whole_spec, whole_spec, whole_spec, whole_spec, whole_spec, whole_spec, whole_spec, whole_spec,
                col_split, col_split, row_split, col_split, col_split, row_split,
                cube_spec, cube_spec, cube_spec)

    def body(hidden_in, cache0, cache1, kv_lens, route_ids, route_wts, att0_q, att0_uk, att0_uv, att0_o, att1_q, att1_uk, att1_uv, att1_o, ffn0_gate, ffn0_up, ffn0_down, ffn1_gate, ffn1_up, ffn1_down, exp_gate, exp_up, exp_down):
        tok, top_k = route_ids.shape
        cap = min(tok, (2 * tok * top_k + n_dev - 1) // n_dev)
        me = lax.axis_index(FLAT_AXES)

        ids_all = route_ids.T[None]
        for mask in (1, 2, 4, 8):
            ids_all = jnp.concatenate([ids_all, xor_send(ids_all, mask)], axis=0)
        wts_grp = route_wts.T[None]
        for mask in (4, 8):
            wts_grp = jnp.concatenate([wts_grp, xor_send(wts_grp, mask)], axis=0)
        slots = jnp.arange(cap)
        hit = jnp.any(ids_all == me, axis=1)
        rank = jnp.where(hit, ranks_of(hit), -1.0).astype(jnp.int32)
        pick = (rank[:, None, :] == slots[None, :, None]).astype(jnp.bfloat16)
        grp_ids = ids_all[::4]
        mine = grp_ids[:, None] == (me ^ jnp.arange(4))[None, :, None, None]
        grp_hit = jnp.any(mine, axis=2)
        grp_rank = jnp.where(grp_hit, ranks_of(grp_hit), -1.0).astype(jnp.int32)
        grp_wt = jnp.sum(jnp.where(mine, wts_grp[:, None], 0.0), axis=2)
        wt_hi = lax.reduce_precision(grp_wt, 8, 7)
        wt_mid = lax.reduce_precision(grp_wt - wt_hi, 8, 7)
        wt_lo = lax.reduce_precision(grp_wt - wt_hi - wt_mid, 8, 7)
        wt_parts = jnp.stack([wt_hi, wt_mid, wt_lo], axis=1)
        spread = jnp.where(grp_rank[:, None, :, :, None] == slots, wt_parts[..., None], 0.0).astype(jnp.bfloat16)
        zero_wt = jnp.sum(jnp.where(route_ids >= n_dev, route_wts, 0.0), axis=1, keepdims=True)

        att_zero = attention(rms_norm(hidden_in), cache0, kv_lens, att0_q, att0_uk, att0_uv, att0_o)
        h_zero = (hidden_in.astype(jnp.float32) + att_zero).astype(jnp.bfloat16)
        u_zero = rms_norm(h_zero)

        grp = gather_tp(u_zero)
        far = [xor_send(rows, 2) for rows in grp]
        near = [xor_send(rows, 1) for rows in grp]
        cross = [xor_send(rows, 1) for rows in far]
        act0 = act_rows(jnp.concatenate(grp, axis=0), ffn0_gate, ffn0_up)
        part0 = jnp.dot(act0, ffn0_down, preferred_element_type=jnp.float32).reshape(4, tok, -1)

        picked = []
        for rel in range(4):
            for rows, sel in zip((grp[rel], near[rel], far[rel], cross[rel]), pick[4 * rel:4 * rel + 4]):
                picked.append(jnp.dot(sel, rows, preferred_element_type=jnp.float32).astype(jnp.bfloat16))
        picked = jnp.concatenate([picked[4 * rel + off] for off in range(4) for rel in range(4)], axis=0)
        picked, part0 = lax.optimization_barrier((picked, part0))
        exp_act = act_rows(picked, exp_gate[0], exp_up[0])
        exp_out = jnp.dot(exp_act, exp_down[0], preferred_element_type=jnp.float32).astype(jnp.bfloat16)
        exp_out = exp_out.reshape(4, 4, cap, -1)
        back = [exp_out[0]] + [xor_send(exp_out[off], off) for off in (1, 2, 3)]

        f_zero = (h_zero.astype(jnp.float32) + reduce_tp(part0)).astype(jnp.bfloat16)
        att_one = attention(rms_norm(f_zero), cache1, kv_lens, att1_q, att1_uk, att1_uv, att1_o)
        h_one = (f_zero.astype(jnp.float32) + att_one).astype(jnp.bfloat16)
        act1 = act_rows(jnp.concatenate(gather_tp(rms_norm(h_one)), axis=0), ffn1_gate, ffn1_up)
        part1 = jnp.dot(act1, ffn1_down, preferred_element_type=jnp.float32).reshape(4, tok, -1)
        for off in range(4):
            for piece in range(3):
                part1 = part1 + jnp.einsum('rtx,rxd->rtd', spread[:, piece, off], back[off], preferred_element_type=jnp.float32)
        total = reduce_tp(part1)
        return (h_one.astype(jnp.float32) + zero_wt * u_zero.astype(jnp.float32) + total).astype(jnp.bfloat16)

    return jax.shard_map(body, mesh=mesh, in_specs=in_specs, out_specs=rows_spec, check_vma=False)
```

```python
import functools

import jax
import jax.numpy as jnp
from jax import lax
from jax.experimental import pallas as pl
from jax.experimental.pallas import tpu as pltpu
from jax.sharding import PartitionSpec as P

FLAT_AXES = ('tp', 'ep')


def rms_norm(vec):
    vec32 = vec.astype(jnp.float32)
    return (vec32 * lax.rsqrt(jnp.mean(vec32 * vec32, axis=-1, keepdims=True) + 1e-6)).astype(jnp.bfloat16)


def rope_rotate(vals, pos):
    half_dim = vals.shape[-1] // 2
    inv_freq = 10000.0 ** (-2.0 * jnp.arange(half_dim, dtype=jnp.float32) / vals.shape[-1])
    rot_angle = pos.astype(jnp.float32)[..., None, None] * inv_freq
    cos_ang = jnp.cos(rot_angle)
    sin_ang = jnp.sin(rot_angle)
    lead_half = vals[..., :half_dim]
    tail_half = vals[..., half_dim:]
    return jnp.concatenate([lead_half * cos_ang - tail_half * sin_ang, tail_half * cos_ang + lead_half * sin_ang], axis=-1)


MESH = pl.DeviceIdType.MESH
NARROW = jnp.bfloat16
WIDE = jnp.float32


def dot_nt(lhs, rhs):
    return lax.dot_general(lhs, rhs, (((1,), (1,)), ((), ())), preferred_element_type=WIDE)


def dot_nn(lhs, rhs):
    return jnp.dot(lhs, rhs, preferred_element_type=WIDE)


def flip(index, mask):
    hi = lax.rem(index // 2 + mask // 2, 2)
    lo = lax.rem(index + mask % 2, 2)
    return hi * 2 + lo


def count_before(hit):
    width = hit.shape[1]
    row = lax.broadcasted_iota(jnp.int32, (width, width), 0)
    col = lax.broadcasted_iota(jnp.int32, (width, width), 1)
    before = jnp.where(row < col, 1.0, 0.0).astype(NARROW)
    return dot_nn(hit.astype(NARROW), before)


def route_kernel(cap, ids_ref, wts_ref, pos_ref, gpos_ref, gwt_ref, ids_in, wts_in, hit_scr, ghit_scr, gwt_scr, send_sem, recv_sem):
    tp, ep = lax.axis_index('tp'), lax.axis_index('ep')
    tok = ids_ref.shape[1]
    barrier = pltpu.get_barrier_semaphore()
    for k in range(1, 16):
        pl.semaphore_signal(barrier, inc=1, device_id=(flip(tp, k // 4), flip(ep, k % 4)), device_id_type=MESH)
    pl.semaphore_wait(barrier, 15)
    copies = []
    for k in range(1, 16):
        peer = (flip(tp, k // 4), flip(ep, k % 4))
        pairs = [(ids_ref, ids_in, 0)] + ([(wts_ref, wts_in, 1)] if k % 4 == 0 else [])
        for src, dst, part in pairs:
            copy = pltpu.make_async_remote_copy(
                src_ref=src, dst_ref=dst.at[k], send_sem=send_sem.at[part, k], recv_sem=recv_sem.at[part, k],
                device_id=peer, device_id_type=MESH)
            copy.start()
            copies.append(copy)
    hit_scr[...] = jnp.zeros_like(hit_scr)
    ghit_scr[...] = jnp.zeros_like(ghit_scr)
    gwt_scr[...] = jnp.zeros_like(gwt_scr)
    for copy in copies:
        copy.wait()
    me = tp * 4 + ep
    for k in range(16):
        ids = ids_ref[...] if k == 0 else ids_in[k]
        hit_scr[k:k + 1, 0:tok] = jnp.sum(jnp.where(ids == me, 1.0, 0.0), axis=0, keepdims=True)
        if k % 4 == 0:
            wts = wts_ref[...] if k == 0 else wts_in[k]
            for s in range(4):
                row = 4 * s + k // 4
                mine = ids == tp * 4 + flip(ep, s)
                ghit_scr[row:row + 1, 0:tok] = jnp.sum(jnp.where(mine, 1.0, 0.0), axis=0, keepdims=True)
                gwt_scr[row:row + 1, 0:tok] = jnp.sum(jnp.where(mine, wts, 0.0), axis=0, keepdims=True)
    rows = lax.broadcasted_iota(jnp.int32, hit_scr.shape, 0)
    hit = hit_scr[...]
    shift = jnp.where((rows // 4) % 2 == 1, 1.0 * cap, 0.0)
    pos_ref[...] = jnp.where(hit > 0.5, count_before(hit) + shift, -1.0).astype(jnp.int32)
    ghit = ghit_scr[...]
    gshift = jnp.where(rows % 2 == 1, 1.0 * cap, 0.0)
    gpos_ref[...] = jnp.where(ghit > 0.5, count_before(ghit) + gshift, -1.0).astype(jnp.int32)
    wts = gwt_scr[...]
    hi = wts.astype(NARROW).astype(WIDE)
    mid = (wts - hi).astype(NARROW).astype(WIDE)
    gwt_ref[0] = hi
    gwt_ref[1] = mid
    gwt_ref[2] = wts - hi - mid


def route_tables(ids_t, wts_t, cap):
    top_k, tok = ids_t.shape
    lanes = 128
    whole = pl.BlockSpec(memory_space=pltpu.VMEM)
    return pl.pallas_call(
        functools.partial(route_kernel, cap),
        out_shape=(jax.ShapeDtypeStruct((16, lanes), jnp.int32), jax.ShapeDtypeStruct((16, lanes), jnp.int32),
                   jax.ShapeDtypeStruct((3, 16, lanes), WIDE)),
        in_specs=[whole, whole],
        out_specs=(whole, whole, whole),
        scratch_shapes=[pltpu.VMEM((16, top_k, tok), jnp.int32), pltpu.VMEM((16, top_k, tok), WIDE),
                        pltpu.VMEM((16, lanes), WIDE), pltpu.VMEM((16, lanes), WIDE), pltpu.VMEM((16, lanes), WIDE),
                        pltpu.SemaphoreType.DMA((2, 16)), pltpu.SemaphoreType.DMA((2, 16))],
        compiler_params=pltpu.CompilerParams(collective_id=1, has_side_effects=True),
        name='route_tables',
    )(ids_t, wts_t)


def ffn_kernel(ff, tile, n_act, with_mix, *refs):
    rows = refs[:4]
    gate_ref, up_ref, down_hbm = refs[4:7]
    mix_ref = refs[7] if with_mix else None
    lead_keep, lead_send, tail_keep, tail_send, x_scr, act_scr, down_scr, sem = refs[7 + with_mix:]
    step = pl.program_id(0)
    tok = rows[0].shape[0]
    last = ff - (n_act - 1) * tile
    last_pad = -(-last // 256) * 256
    n_col = down_scr.shape[0]
    cols = down_scr.shape[2]

    def down_copy(c):
        return pltpu.make_async_copy(down_hbm.at[:, c * cols:(c + 1) * cols], down_scr.at[c, 0:ff, :], sem.at[c])

    @pl.when(step == 0)
    def _():
        for r in range(4):
            x_scr[r * tok:(r + 1) * tok, :] = rows[r][...]
        for c in range(n_col):
            down_scr[c, ff:, :] = jnp.zeros((down_scr.shape[1] - ff, cols), NARROW)

    for c in range(n_col):
        @pl.when(step == c + 1)
        def _():
            down_copy(c).start()

    def act_of(width):
        gate_val = dot_nt(x_scr[...], gate_ref[0:width, :])
        up_val = dot_nt(x_scr[...], up_ref[0:width, :])
        return jax.nn.silu(gate_val) * up_val

    @pl.when(step < n_act - 1)
    def _():
        act_scr[:, pl.ds(pl.multiple_of(step * tile, tile), tile)] = act_of(tile).astype(NARROW)

    @pl.when(step == n_act - 1)
    def _():
        act = act_of(last_pad)
        live = lax.broadcasted_iota(jnp.int32, act.shape, 1) < last
        act_scr[:, (n_act - 1) * tile:] = jnp.where(live, act, 0.0).astype(NARROW)

    for c in range(n_col):
        @pl.when(step == n_act + c)
        def _():
            down_copy(c).wait()
            out = dot_nn(act_scr[...], down_scr[c])
            if with_mix:
                out = out + mix_ref[...]
            if c < n_col // 2:
                lead_keep[...] = out[:2 * tok]
                lead_send[...] = out[2 * tok:]
            else:
                tail_keep[0:tok, :] = out[:tok]
                tail_keep[tok:, :] = out[2 * tok:3 * tok]
                tail_send[0:tok, :] = out[tok:2 * tok]
                tail_send[tok:, :] = out[3 * tok:]


def dense_partial(rows, w_gate, w_up, w_down, mix=None):
    tok, hidden = rows[0].shape
    ff = w_down.shape[0]
    tile, cols = 512, 512
    n_act = -(-ff // tile)
    n_col = hidden // cols
    ff_pad = (n_act - 1) * tile + -(-(ff - (n_act - 1) * tile) // 256) * 256
    whole = pl.BlockSpec((tok, hidden), lambda i: (0, 0))
    weight = pl.BlockSpec((tile, hidden), lambda i: (jnp.minimum(i, n_act - 1), 0))
    half = n_col // 2
    lead = pl.BlockSpec((2 * tok, cols), lambda i: (0, jnp.clip(i - n_act, 0, half - 1)))
    tail = pl.BlockSpec((2 * tok, cols), lambda i: (0, jnp.clip(i - n_act - half, 0, half - 1)))
    args = [*rows, w_gate.T, w_up.T, w_down]
    in_specs = [whole] * 4 + [weight, weight, pl.BlockSpec(memory_space=pl.ANY)]
    if mix is not None:
        args.append(mix)
        in_specs.append(pl.BlockSpec((4 * tok, cols), lambda i: (0, jnp.clip(i - n_act, 0, n_col - 1))))
    out = jax.ShapeDtypeStruct((2 * tok, hidden // 2), WIDE)
    return pl.pallas_call(
        functools.partial(ffn_kernel, ff, tile, n_act, int(mix is not None)),
        out_shape=(out,) * 4,
        grid=(n_act + n_col,),
        in_specs=in_specs,
        out_specs=(lead, lead, tail, tail),
        scratch_shapes=[pltpu.VMEM((4 * tok, hidden), NARROW), pltpu.VMEM((4 * tok, ff_pad), NARROW),
                        pltpu.VMEM((n_col, ff_pad, cols), NARROW), pltpu.SemaphoreType.DMA((n_col,))],
        cost_estimate=pl.CostEstimate(flops=6 * 4 * tok * hidden * ff, bytes_accessed=6 * hidden * ff, transcendentals=0),
        name='dense_partial',
    )(*args)


def expert_kernel(cap, tile, n_act, pos_ref, *refs):
    blocks = refs[:16]
    gate_ref, up_ref, down_ref = refs[16:19]
    outs = refs[19:23]
    u_scr, x_scr, act_scr, sem = refs[23:]
    step = pl.program_id(0)
    tok = blocks[0].shape[0]
    width = u_scr.shape[2]
    ff = down_ref.shape[0]

    @pl.when(step == 0)
    def _():
        copies = []
        for k in range(16):
            copy = pltpu.make_async_copy(blocks[k], u_scr.at[k % 4, k // 4, 0:tok, :], sem.at[k])
            copy.start()
            copies.append(copy)
        u_scr[:, :, tok:, :] = jnp.zeros((4, 4, width - tok, u_scr.shape[3]), NARROW)
        for copy in copies:
            copy.wait()
        slot = lax.broadcasted_iota(jnp.int32, (2 * cap, width), 0)
        for s in range(4):
            for p in range(2):
                pick = jnp.concatenate(
                    [jnp.where(slot == pos_ref[pl.ds(4 * r + s, 1), :], 1.0, 0.0) for r in (2 * p, 2 * p + 1)], axis=1)
                pair = u_scr[s, 2 * p:2 * p + 2].reshape(2 * width, -1)
                x_scr[s, 2 * cap * p:2 * cap * (p + 1), :] = dot_nn(pick.astype(NARROW), pair).astype(NARROW)

    @pl.when(step < n_act)
    def _():
        def one(s, carry):
            gate_val = dot_nn(x_scr[s], gate_ref[...])
            up_val = dot_nn(x_scr[s], up_ref[...])
            act = (jax.nn.silu(gate_val) * up_val).astype(NARROW)
            act_scr[s, :, pl.ds(pl.multiple_of(step * tile, tile), tile)] = act
            return carry
        lax.fori_loop(0, 4, one, 0)

    @pl.when(step >= n_act)
    def _():
        for s in range(4):
            outs[s][...] = dot_nn(act_scr[s, :, 0:ff], down_ref[...]).astype(NARROW)


def expert_rows(pos, blocks, w_gate, w_up, w_down, cap):
    tok, hidden = blocks[0].shape
    ff = w_down.shape[0]
    tile, cols = 512, 512
    n_act = -(-ff // tile)
    n_col = hidden // cols
    anywhere = pl.BlockSpec(memory_space=pl.ANY)
    weight = pl.BlockSpec((hidden, tile), lambda i: (0, jnp.minimum(i, n_act - 1)))
    down = pl.BlockSpec((ff, cols), lambda i: (0, jnp.clip(i - n_act, 0, n_col - 1)))
    out = pl.BlockSpec((4 * cap, cols), lambda i: (0, jnp.clip(i - n_act, 0, n_col - 1)))
    return pl.pallas_call(
        functools.partial(expert_kernel, cap, tile, n_act),
        out_shape=(jax.ShapeDtypeStruct((4 * cap, hidden), NARROW),) * 4,
        grid=(n_act + n_col,),
        in_specs=[pl.BlockSpec(pos.shape, lambda i: (0, 0))] + [anywhere] * 16 + [weight, weight, down],
        out_specs=(out,) * 4,
        scratch_shapes=[pltpu.VMEM((4, 4, 128, hidden), NARROW), pltpu.VMEM((4, 4 * cap, hidden), NARROW),
                        pltpu.VMEM((4, 4 * cap, n_act * tile), NARROW), pltpu.SemaphoreType.DMA((16,))],
        cost_estimate=pl.CostEstimate(flops=6 * 16 * cap * hidden * ff, bytes_accessed=6 * hidden * ff, transcendentals=0),
        name='expert_rows',
    )(pos, *blocks, w_gate, w_up, w_down)


def mix_kernel(cap, tok, gpos_ref, gwt_ref, *refs):
    back = refs[:4]
    out_ref, spread = refs[4:]
    lanes = gpos_ref.shape[1]
    step = pl.program_id(0)

    @pl.when(step == 0)
    def _():
        slot = lax.broadcasted_iota(jnp.int32, (2 * cap, lanes), 0)
        for p in range(2):
            for s in range(4):
                for half in range(2):
                    row = 4 * s + 2 * p + half
                    hit = slot == gpos_ref[row:row + 1, :]
                    for part in range(3):
                        val = jnp.where(hit, gwt_ref[part, row:row + 1, :], 0.0).astype(NARROW)
                        col = (2 * part + half) * lanes
                        spread[p, 2 * cap * s:2 * cap * (s + 1), col:col + lanes] = val

    for p in range(2):
        rhs = jnp.concatenate([ref[2 * cap * p:2 * cap * (p + 1), :] for ref in back], axis=0)
        res = lax.dot_general(spread[p], rhs, (((0,), (0,)), ((), ())), preferred_element_type=WIDE)
        res = res[0:2 * lanes] + res[2 * lanes:4 * lanes] + res[4 * lanes:6 * lanes]
        out_ref[2 * p * tok:(2 * p + 1) * tok, :] = res[0:tok]
        out_ref[(2 * p + 1) * tok:(2 * p + 2) * tok, :] = res[lanes:lanes + tok]


def mix_rows(gpos, gwt, back, tok, cap):
    hidden = back[0].shape[1]
    cols = 512
    return pl.pallas_call(
        functools.partial(mix_kernel, cap, tok),
        out_shape=jax.ShapeDtypeStruct((4 * tok, hidden), WIDE),
        grid=(hidden // cols,),
        in_specs=[pl.BlockSpec(gpos.shape, lambda i: (0, 0)), pl.BlockSpec(gwt.shape, lambda i: (0, 0, 0))]
        + [pl.BlockSpec((4 * cap, cols), lambda i: (0, i))] * 4,
        out_specs=pl.BlockSpec((4 * tok, cols), lambda i: (0, i)),
        scratch_shapes=[pltpu.VMEM((2, 8 * cap, 6 * gpos.shape[1]), NARROW)],
        cost_estimate=pl.CostEstimate(flops=4 * 3 * 256 * 8 * cap * hidden, bytes_accessed=32 * cap * hidden, transcendentals=0),
        name='mix_rows',
    )(gpos, gwt, *back)


def attention(normed, cache, kv_lens, w_q, w_uk, w_uv, w_o):
    nope_dim = w_uk.shape[1]
    latent = w_uk.shape[2]
    scale = w_q.shape[2] ** -0.5
    q_full = jnp.einsum('bd,dhc->bhc', normed, w_q, preferred_element_type=jnp.float32).astype(jnp.bfloat16)
    q_rope = rope_rotate(q_full[..., nope_dim:].astype(jnp.float32), kv_lens).astype(jnp.bfloat16)
    q_lat = jnp.einsum('bhn,hnl->bhl', q_full[..., :nope_dim], w_uk, preferred_element_type=jnp.float32).astype(jnp.bfloat16)
    q_cat = jnp.concatenate([q_lat, q_rope], axis=-1)
    scores = jnp.einsum('bhc,bpc->bhp', q_cat, cache, preferred_element_type=jnp.float32) * scale
    valid = jnp.arange(cache.shape[1])[None, None, :] < kv_lens[:, None, None]
    probs = jax.nn.softmax(jnp.where(valid, scores, -1e30), axis=-1).astype(jnp.bfloat16)
    o_lat = jnp.einsum('bhp,bpl->bhl', probs, cache[:, :, :latent], preferred_element_type=jnp.float32).astype(jnp.bfloat16)
    o_val = jnp.einsum('bhl,hlv->bhv', o_lat, w_uv, preferred_element_type=jnp.float32).astype(jnp.bfloat16)
    return jnp.einsum('bhv,hvd->bd', o_val, w_o, preferred_element_type=jnp.float32)


def xor_send(vals, mask):
    return lax.ppermute(vals, FLAT_AXES, [(dev, dev ^ mask) for dev in range(16)])


def gather_tp(rows):
    return [rows] + [xor_send(rows, 4 * rel) for rel in (1, 2, 3)]


def reduce_tp(lead_keep, lead_send, tail_keep, tail_send):
    tok = lead_keep.shape[0] // 2
    lead_in = xor_send(lead_send, 8)
    tail_in = xor_send(tail_send, 4)
    lead_far = xor_send(lead_keep[tok:] + lead_in[tok:], 4)
    tail_far = xor_send(tail_keep[tok:] + tail_in[tok:], 8)
    lead_own = lead_keep[:tok] + lead_in[:tok] + lead_far
    tail_own = tail_keep[:tok] + tail_in[:tok] + tail_far
    return jnp.concatenate([lead_own, tail_own], axis=-1)


def solution(mesh):
    n_dev = mesh.shape['tp'] * mesh.shape['ep']
    rows_spec = P(FLAT_AXES, None)
    cube_spec = P(FLAT_AXES, None, None)
    whole_spec = P(None, None, None)
    col_split = P(None, 'tp')
    row_split = P('tp', None)
    in_specs = (rows_spec, cube_spec, cube_spec, P(FLAT_AXES), rows_spec, rows_spec,
                whole_spec, whole_spec, whole_spec, whole_spec, whole_spec, whole_spec, whole_spec, whole_spec,
                col_split, col_split, row_split, col_split, col_split, row_split,
                cube_spec, cube_spec, cube_spec)

    def body(hidden_in, cache0, cache1, kv_lens, route_ids, route_wts, att0_q, att0_uk, att0_uv, att0_o, att1_q, att1_uk, att1_uv, att1_o, ffn0_gate, ffn0_up, ffn0_down, ffn1_gate, ffn1_up, ffn1_down, exp_gate, exp_up, exp_down):
        tok, top_k = route_ids.shape
        cap = min(tok, (2 * tok * top_k + n_dev - 1) // n_dev)
        pos, gpos, gwt = route_tables(route_ids.T, route_wts.T, cap)
        zero_wt = jnp.sum(jnp.where(route_ids >= n_dev, route_wts, 0.0), axis=1, keepdims=True)

        att_zero = attention(rms_norm(hidden_in), cache0, kv_lens, att0_q, att0_uk, att0_uv, att0_o)
        h_zero = (hidden_in.astype(jnp.float32) + att_zero).astype(jnp.bfloat16)
        u_zero = rms_norm(h_zero)

        grp = gather_tp(u_zero)
        far = [xor_send(rows, 2) for rows in grp]
        near = [xor_send(rows, 1) for rows in grp]
        cross = [xor_send(rows, 1) for rows in far]
        part0 = dense_partial(grp, ffn0_gate, ffn0_up, ffn0_down)
        blocks = [rows for rel in range(4) for rows in (grp[rel], near[rel], far[rel], cross[rel])]
        pos, part0 = lax.optimization_barrier((pos, part0))
        exp_out = expert_rows(pos, blocks, exp_gate[0], exp_up[0], exp_down[0], cap)
        back = [exp_out[0]] + [xor_send(exp_out[off], off) for off in (1, 2, 3)]

        f_zero = (h_zero.astype(jnp.float32) + reduce_tp(*part0)).astype(jnp.bfloat16)
        att_one = attention(rms_norm(f_zero), cache1, kv_lens, att1_q, att1_uk, att1_uv, att1_o)
        h_one = (f_zero.astype(jnp.float32) + att_one).astype(jnp.bfloat16)
        grp1 = gather_tp(rms_norm(h_one))
        mix = mix_rows(gpos, gwt, back, tok, cap)
        part1 = dense_partial(grp1, ffn1_gate, ffn1_up, ffn1_down, mix)
        total = reduce_tp(*part1)
        return (h_one.astype(jnp.float32) + zero_wt * u_zero.astype(jnp.float32) + total).astype(jnp.bfloat16)

    return jax.shard_map(body, mesh=mesh, in_specs=in_specs, out_specs=rows_spec, check_vma=False)
```

```python
import functools

import jax
import jax.numpy as jnp
from jax import lax
from jax.experimental import pallas as pl
from jax.experimental.pallas import tpu as pltpu
from jax.sharding import PartitionSpec as P

FLAT_AXES = ('tp', 'ep')
MESH = pl.DeviceIdType.MESH
NARROW = jnp.bfloat16
WIDE = jnp.float32


def dot_nt(lhs, rhs):
    return lax.dot_general(lhs, rhs, (((1,), (1,)), ((), ())), preferred_element_type=WIDE)


def dot_nn(lhs, rhs):
    return jnp.dot(lhs, rhs, preferred_element_type=WIDE)


def flip(index, mask):
    hi = lax.rem(index // 2 + mask // 2, 2)
    lo = lax.rem(index + mask % 2, 2)
    return hi * 2 + lo


def count_before(hit):
    width = hit.shape[1]
    row = lax.broadcasted_iota(jnp.int32, (width, width), 0)
    col = lax.broadcasted_iota(jnp.int32, (width, width), 1)
    before = jnp.where(row < col, 1.0, 0.0).astype(NARROW)
    return dot_nn(hit.astype(NARROW), before)


def route_kernel(cap, ids_ref, wts_ref, pos_ref, gpos_ref, gwt_ref, ids_in, wts_in, hit_scr, ghit_scr, gwt_scr, send_sem, recv_sem):
    tp, ep = lax.axis_index('tp'), lax.axis_index('ep')
    tok = ids_ref.shape[1]
    barrier = pltpu.get_barrier_semaphore()
    for k in range(1, 16):
        pl.semaphore_signal(barrier, inc=1, device_id=(flip(tp, k // 4), flip(ep, k % 4)), device_id_type=MESH)
    pl.semaphore_wait(barrier, 15)
    copies = []
    for k in range(1, 16):
        peer = (flip(tp, k // 4), flip(ep, k % 4))
        pairs = [(ids_ref, ids_in, 0)] + ([(wts_ref, wts_in, 1)] if k % 4 == 0 else [])
        for src, dst, part in pairs:
            copy = pltpu.make_async_remote_copy(
                src_ref=src, dst_ref=dst.at[k], send_sem=send_sem.at[part, k], recv_sem=recv_sem.at[part, k],
                device_id=peer, device_id_type=MESH)
            copy.start()
            copies.append(copy)
    hit_scr[...] = jnp.zeros_like(hit_scr)
    ghit_scr[...] = jnp.zeros_like(ghit_scr)
    gwt_scr[...] = jnp.zeros_like(gwt_scr)
    for copy in copies:
        copy.wait()
    me = tp * 4 + ep
    for k in range(16):
        ids = ids_ref[...] if k == 0 else ids_in[k]
        hit_scr[k:k + 1, 0:tok] = jnp.sum(jnp.where(ids == me, 1.0, 0.0), axis=0, keepdims=True)
        if k % 4 == 0:
            wts = wts_ref[...] if k == 0 else wts_in[k]
            for s in range(4):
                row = 4 * s + k // 4
                mine = ids == tp * 4 + flip(ep, s)
                ghit_scr[row:row + 1, 0:tok] = jnp.sum(jnp.where(mine, 1.0, 0.0), axis=0, keepdims=True)
                gwt_scr[row:row + 1, 0:tok] = jnp.sum(jnp.where(mine, wts, 0.0), axis=0, keepdims=True)
    rows = lax.broadcasted_iota(jnp.int32, hit_scr.shape, 0)
    hit = hit_scr[...]
    shift = jnp.where((rows // 4) % 2 == 1, 1.0 * cap, 0.0)
    pos_ref[...] = jnp.where(hit > 0.5, count_before(hit) + shift, -1.0).astype(jnp.int32)
    ghit = ghit_scr[...]
    gshift = jnp.where(rows % 2 == 1, 1.0 * cap, 0.0)
    gpos_ref[...] = jnp.where(ghit > 0.5, count_before(ghit) + gshift, -1.0).astype(jnp.int32)
    wts = gwt_scr[...]
    hi = wts.astype(NARROW).astype(WIDE)
    mid = (wts - hi).astype(NARROW).astype(WIDE)
    gwt_ref[0] = hi
    gwt_ref[1] = mid
    gwt_ref[2] = wts - hi - mid


def route_tables(ids_t, wts_t, cap):
    top_k, tok = ids_t.shape
    lanes = 128
    whole = pl.BlockSpec(memory_space=pltpu.VMEM)
    return pl.pallas_call(
        functools.partial(route_kernel, cap),
        out_shape=(jax.ShapeDtypeStruct((16, lanes), jnp.int32), jax.ShapeDtypeStruct((16, lanes), jnp.int32),
                   jax.ShapeDtypeStruct((3, 16, lanes), WIDE)),
        in_specs=[whole, whole],
        out_specs=(whole, whole, whole),
        scratch_shapes=[pltpu.VMEM((16, top_k, tok), jnp.int32), pltpu.VMEM((16, top_k, tok), WIDE),
                        pltpu.VMEM((16, lanes), WIDE), pltpu.VMEM((16, lanes), WIDE), pltpu.VMEM((16, lanes), WIDE),
                        pltpu.SemaphoreType.DMA((2, 16)), pltpu.SemaphoreType.DMA((2, 16))],
        compiler_params=pltpu.CompilerParams(collective_id=1, has_side_effects=True),
        name='route_tables',
    )(ids_t, wts_t)


def ffn_kernel(ff, tile, n_act, with_mix, *refs):
    rows = refs[:4]
    gate_ref, up_ref, down_hbm = refs[4:7]
    mix_ref = refs[7] if with_mix else None
    lead_keep, lead_send, tail_keep, tail_send, x_scr, act_scr, down_scr, sem = refs[7 + with_mix:]
    step = pl.program_id(0)
    tok = rows[0].shape[0]
    last = ff - (n_act - 1) * tile
    last_pad = -(-last // 256) * 256
    n_col = down_scr.shape[0]
    cols = down_scr.shape[2]

    def down_copy(c):
        return pltpu.make_async_copy(down_hbm.at[:, c * cols:(c + 1) * cols], down_scr.at[c, 0:ff, :], sem.at[c])

    @pl.when(step == 0)
    def _():
        for r in range(4):
            x_scr[r * tok:(r + 1) * tok, :] = rows[r][...]
        for c in range(n_col):
            down_scr[c, ff:, :] = jnp.zeros((down_scr.shape[1] - ff, cols), NARROW)

    for c in range(n_col):
        @pl.when(step == c + 1)
        def _():
            down_copy(c).start()

    def act_of(width):
        gate_val = dot_nt(x_scr[...], gate_ref[0:width, :])
        up_val = dot_nt(x_scr[...], up_ref[0:width, :])
        return jax.nn.silu(gate_val) * up_val

    @pl.when(step < n_act - 1)
    def _():
        act_scr[:, pl.ds(pl.multiple_of(step * tile, tile), tile)] = act_of(tile).astype(NARROW)

    @pl.when(step == n_act - 1)
    def _():
        act = act_of(last_pad)
        live = lax.broadcasted_iota(jnp.int32, act.shape, 1) < last
        act_scr[:, (n_act - 1) * tile:] = jnp.where(live, act, 0.0).astype(NARROW)

    for c in range(n_col):
        @pl.when(step == n_act + c)
        def _():
            down_copy(c).wait()
            out = dot_nn(act_scr[...], down_scr[c])
            if with_mix:
                out = out + mix_ref[...]
            if c < n_col // 2:
                lead_keep[...] = out[:2 * tok]
                lead_send[...] = out[2 * tok:]
            else:
                tail_keep[0:tok, :] = out[:tok]
                tail_keep[tok:, :] = out[2 * tok:3 * tok]
                tail_send[0:tok, :] = out[tok:2 * tok]
                tail_send[tok:, :] = out[3 * tok:]


def dense_partial(rows, w_gate, w_up, w_down, mix=None):
    tok, hidden = rows[0].shape
    ff = w_down.shape[0]
    tile, cols = 512, 512
    n_act = -(-ff // tile)
    n_col = hidden // cols
    ff_pad = (n_act - 1) * tile + -(-(ff - (n_act - 1) * tile) // 256) * 256
    whole = pl.BlockSpec((tok, hidden), lambda i: (0, 0))
    weight = pl.BlockSpec((tile, hidden), lambda i: (jnp.minimum(i, n_act - 1), 0))
    half = n_col // 2
    lead = pl.BlockSpec((2 * tok, cols), lambda i: (0, jnp.clip(i - n_act, 0, half - 1)))
    tail = pl.BlockSpec((2 * tok, cols), lambda i: (0, jnp.clip(i - n_act - half, 0, half - 1)))
    args = [*rows, w_gate.T, w_up.T, w_down]
    in_specs = [whole] * 4 + [weight, weight, pl.BlockSpec(memory_space=pl.ANY)]
    if mix is not None:
        args.append(mix)
        in_specs.append(pl.BlockSpec((4 * tok, cols), lambda i: (0, jnp.clip(i - n_act, 0, n_col - 1))))
    out = jax.ShapeDtypeStruct((2 * tok, hidden // 2), WIDE)
    return pl.pallas_call(
        functools.partial(ffn_kernel, ff, tile, n_act, int(mix is not None)),
        out_shape=(out,) * 4,
        grid=(n_act + n_col,),
        in_specs=in_specs,
        out_specs=(lead, lead, tail, tail),
        scratch_shapes=[pltpu.VMEM((4 * tok, hidden), NARROW), pltpu.VMEM((4 * tok, ff_pad), NARROW),
                        pltpu.VMEM((n_col, ff_pad, cols), NARROW), pltpu.SemaphoreType.DMA((n_col,))],
        cost_estimate=pl.CostEstimate(flops=6 * 4 * tok * hidden * ff, bytes_accessed=6 * hidden * ff, transcendentals=0),
        name='dense_partial',
    )(*args)


def expert_kernel(cap, tile, n_act, pos_ref, *refs):
    blocks = refs[:16]
    gate_ref, up_ref, down_ref = refs[16:19]
    outs = refs[19:23]
    u_scr, x_scr, act_scr, sem = refs[23:]
    step = pl.program_id(0)
    tok = blocks[0].shape[0]
    width = u_scr.shape[2]
    ff = down_ref.shape[0]

    @pl.when(step == 0)
    def _():
        copies = []
        for k in range(16):
            copy = pltpu.make_async_copy(blocks[k], u_scr.at[k % 4, k // 4, 0:tok, :], sem.at[k])
            copy.start()
            copies.append(copy)
        u_scr[:, :, tok:, :] = jnp.zeros((4, 4, width - tok, u_scr.shape[3]), NARROW)
        for copy in copies:
            copy.wait()
        slot = lax.broadcasted_iota(jnp.int32, (2 * cap, width), 0)
        for s in range(4):
            for p in range(2):
                pick = jnp.concatenate(
                    [jnp.where(slot == pos_ref[pl.ds(4 * r + s, 1), :], 1.0, 0.0) for r in (2 * p, 2 * p + 1)], axis=1)
                pair = u_scr[s, 2 * p:2 * p + 2].reshape(2 * width, -1)
                x_scr[s, 2 * cap * p:2 * cap * (p + 1), :] = dot_nn(pick.astype(NARROW), pair).astype(NARROW)

    @pl.when(step < n_act)
    def _():
        def one(s, carry):
            gate_val = dot_nn(x_scr[s], gate_ref[...])
            up_val = dot_nn(x_scr[s], up_ref[...])
            act = (jax.nn.silu(gate_val) * up_val).astype(NARROW)
            act_scr[s, :, pl.ds(pl.multiple_of(step * tile, tile), tile)] = act
            return carry

        lax.fori_loop(0, 4, one, 0)

    @pl.when(step >= n_act)
    def _():
        for s in range(4):
            outs[s][...] = dot_nn(act_scr[s, :, 0:ff], down_ref[...]).astype(NARROW)


def expert_rows(pos, blocks, w_gate, w_up, w_down, cap):
    _, hidden = blocks[0].shape
    ff = w_down.shape[0]
    tile, cols = 512, 512
    n_act = -(-ff // tile)
    n_col = hidden // cols
    anywhere = pl.BlockSpec(memory_space=pl.ANY)
    weight = pl.BlockSpec((hidden, tile), lambda i: (0, jnp.minimum(i, n_act - 1)))
    down = pl.BlockSpec((ff, cols), lambda i: (0, jnp.clip(i - n_act, 0, n_col - 1)))
    out = pl.BlockSpec((4 * cap, cols), lambda i: (0, jnp.clip(i - n_act, 0, n_col - 1)))
    return pl.pallas_call(
        functools.partial(expert_kernel, cap, tile, n_act),
        out_shape=(jax.ShapeDtypeStruct((4 * cap, hidden), NARROW),) * 4,
        grid=(n_act + n_col,),
        in_specs=[pl.BlockSpec(pos.shape, lambda i: (0, 0))] + [anywhere] * 16 + [weight, weight, down],
        out_specs=(out,) * 4,
        scratch_shapes=[pltpu.VMEM((4, 4, 128, hidden), NARROW), pltpu.VMEM((4, 4 * cap, hidden), NARROW),
                        pltpu.VMEM((4, 4 * cap, n_act * tile), NARROW), pltpu.SemaphoreType.DMA((16,))],
        cost_estimate=pl.CostEstimate(flops=6 * 16 * cap * hidden * ff, bytes_accessed=6 * hidden * ff, transcendentals=0),
        name='expert_rows',
    )(pos, *blocks, w_gate, w_up, w_down)


def mix_kernel(cap, tok, gpos_ref, gwt_ref, *refs):
    back = refs[:4]
    out_ref, spread = refs[4:]
    lanes = gpos_ref.shape[1]
    step = pl.program_id(0)

    @pl.when(step == 0)
    def _():
        slot = lax.broadcasted_iota(jnp.int32, (2 * cap, lanes), 0)
        for p in range(2):
            for s in range(4):
                for half in range(2):
                    row = 4 * s + 2 * p + half
                    hit = slot == gpos_ref[row:row + 1, :]
                    for part in range(3):
                        val = jnp.where(hit, gwt_ref[part, row:row + 1, :], 0.0).astype(NARROW)
                        col = (2 * part + half) * lanes
                        spread[p, 2 * cap * s:2 * cap * (s + 1), col:col + lanes] = val

    for p in range(2):
        rhs = jnp.concatenate([ref[2 * cap * p:2 * cap * (p + 1), :] for ref in back], axis=0)
        res = lax.dot_general(spread[p], rhs, (((0,), (0,)), ((), ())), preferred_element_type=WIDE)
        res = res[0:2 * lanes] + res[2 * lanes:4 * lanes] + res[4 * lanes:6 * lanes]
        out_ref[2 * p * tok:(2 * p + 1) * tok, :] = res[0:tok]
        out_ref[(2 * p + 1) * tok:(2 * p + 2) * tok, :] = res[lanes:lanes + tok]


def mix_rows(gpos, gwt, back, tok, cap):
    hidden = back[0].shape[1]
    cols = 512
    return pl.pallas_call(
        functools.partial(mix_kernel, cap, tok),
        out_shape=jax.ShapeDtypeStruct((4 * tok, hidden), WIDE),
        grid=(hidden // cols,),
        in_specs=[pl.BlockSpec(gpos.shape, lambda i: (0, 0)), pl.BlockSpec(gwt.shape, lambda i: (0, 0, 0))]
        + [pl.BlockSpec((4 * cap, cols), lambda i: (0, i))] * 4,
        out_specs=pl.BlockSpec((4 * tok, cols), lambda i: (0, i)),
        scratch_shapes=[pltpu.VMEM((2, 8 * cap, 6 * gpos.shape[1]), NARROW)],
        cost_estimate=pl.CostEstimate(flops=4 * 3 * 256 * 8 * cap * hidden, bytes_accessed=32 * cap * hidden, transcendentals=0),
        name='mix_rows',
    )(gpos, gwt, *back)


def row_norm(vec32):
    return (vec32 * lax.rsqrt(jnp.mean(vec32 * vec32, axis=-1, keepdims=True) + 1e-6)).astype(NARROW)


def attention_kernel(scale, n_q, n_tok, lens_ref, x_ref, wq_ref, uk_ref, cos_ref, sin_ref, cache_ref, uv_hbm, wo_hbm,
                     res_ref, norm_ref, xn_scr, ql_scr, qr_scr, o_scr, ov_scr, uv_scr, wo_scr, sem):
    step = pl.program_id(0)
    heads = uk_ref.shape[0]
    nope, latent = uk_ref.shape[1], uk_ref.shape[2]
    width = wq_ref.shape[0] // heads
    rope = width - nope
    group = cache_ref.shape[0]
    span = cache_ref.shape[2]
    tok = x_ref.shape[0]
    n_head = uv_scr.shape[0]
    value = uv_scr.shape[2]
    uv_copy = pltpu.make_async_copy(uv_hbm, uv_scr, sem.at[0])
    wo_copy = pltpu.make_async_copy(wo_hbm, wo_scr, sem.at[1])

    @pl.when(step == 0)
    def _():
        xn_scr[...] = row_norm(x_ref[...].astype(WIDE))

    @pl.when(step == n_q - 1)
    def _():
        uv_copy.start()
        wo_copy.start()

    for i in range(n_q):
        @pl.when(step == i)
        def _():
            xn = xn_scr[...]
            for a in range(0, heads, 2):
                w_pair = jnp.concatenate([wq_ref[width * g:width * g + nope, :] for g in (a, a + 1)], axis=0)
                q_pair = dot_nt(xn, w_pair).astype(NARROW)
                for j in range(2):
                    q_lat = dot_nn(q_pair[:, nope * j:nope * (j + 1)], uk_ref[a + j])
                    ql_scr[:, heads * i + a + j, :] = q_lat.astype(NARROW).astype(WIDE)
            w_rope = jnp.concatenate([wq_ref[width * g + nope:width * (g + 1), :] for g in range(heads)], axis=0)
            q_rope = dot_nt(xn, w_rope).astype(NARROW).astype(WIDE)
            lane = lax.broadcasted_iota(jnp.int32, q_rope.shape, 1)
            other = jnp.where(lane % rope < rope // 2, pltpu.roll(q_rope, heads * rope - rope // 2, 1),
                              pltpu.roll(q_rope, rope // 2, 1))
            turned = q_rope * cos_ref[...] + other * sin_ref[...]
            turned = turned.astype(NARROW).astype(WIDE)
            for g in range(heads):
                qr_scr[:, heads * i + g, :] = turned[:, rope * g:rope * (g + 1)]

    @pl.when((step >= n_q) & (step < n_q + n_tok))
    def _():
        block = step - n_q
        for k in range(group):
            t = block * group + k
            score = dot_nn(ql_scr[t].astype(NARROW), cache_ref[k, 0:latent, :])
            score = score + dot_nn(qr_scr[t].astype(NARROW), cache_ref[k, latent:latent + rope, :])
            live = lax.broadcasted_iota(jnp.int32, (n_head, span), 1) < lens_ref[t]
            score = jnp.where(live, score * scale, -1e30)
            top = jnp.max(score, axis=-1, keepdims=True)
            weight = jnp.exp(score - top)
            prob = (weight / jnp.sum(weight, axis=-1, keepdims=True)).astype(NARROW)
            o_scr[block, :, k, :] = dot_nt(prob, cache_ref[k, 0:latent, :])

    @pl.when(step == n_q + n_tok)
    def _():
        uv_copy.wait()
        for h in range(n_head):
            o_lat = o_scr[:, h, :, :].reshape(tok, latent).astype(NARROW)
            ov_scr[:, value * h:value * (h + 1)] = dot_nn(o_lat, uv_scr[h]).astype(NARROW)
        wo_copy.wait()
        total = (x_ref[...].astype(WIDE) + dot_nn(ov_scr[...], wo_scr[...])).astype(NARROW)
        res_ref[...] = total
        norm_ref[...] = row_norm(total.astype(WIDE))


def rotary_tables(kv_lens, rope, heads):
    half = rope // 2
    inv_freq = 10000.0 ** (-2.0 * jnp.arange(half, dtype=WIDE) / rope)
    angle = kv_lens.astype(WIDE)[:, None] * inv_freq
    cos_ang, sin_ang = jnp.cos(angle), jnp.sin(angle)
    return jnp.tile(cos_ang, (1, 2 * heads)), jnp.tile(jnp.concatenate([-sin_ang, sin_ang], axis=1), (1, heads))


def attention(x, cache, kv_lens, tables, w_q, w_uk, w_uv, w_o):
    tok, hidden = x.shape
    n_head, nope, latent = w_uk.shape
    width = w_q.shape[2]
    value = w_uv.shape[2]
    span = cache.shape[1]
    heads, group = 4, 8
    n_q, n_tok = n_head // heads, tok // group
    whole = lambda shape: pl.BlockSpec(shape, lambda i, lens: (0,) * len(shape))
    anywhere = pl.BlockSpec(memory_space=pl.ANY)
    out = jax.ShapeDtypeStruct((tok, hidden), NARROW)
    grid_spec = pltpu.PrefetchScalarGridSpec(
        num_scalar_prefetch=1,
        grid=(n_q + n_tok + 1,),
        in_specs=[whole((tok, hidden)),
                  pl.BlockSpec((heads * width, hidden), lambda i, lens: (jnp.minimum(i, n_q - 1), 0)),
                  pl.BlockSpec((heads, nope, latent), lambda i, lens: (jnp.minimum(i, n_q - 1), 0, 0)),
                  whole(tables[0].shape), whole(tables[1].shape),
                  pl.BlockSpec((group, latent + width - nope, span), lambda i, lens: (jnp.clip(i - n_q, 0, n_tok - 1), 0, 0)),
                  anywhere, anywhere],
        out_specs=(whole((tok, hidden)), whole((tok, hidden))),
        scratch_shapes=[pltpu.VMEM((tok, hidden), NARROW), pltpu.VMEM((tok, n_head, latent), WIDE),
                        pltpu.VMEM((tok, n_head, width - nope), WIDE), pltpu.VMEM((n_tok, n_head, group, latent), WIDE),
                        pltpu.VMEM((tok, n_head * value), NARROW), pltpu.VMEM(w_uv.shape, NARROW),
                        pltpu.VMEM((n_head * value, hidden), NARROW), pltpu.SemaphoreType.DMA((2,))])
    flops = 2 * tok * (hidden * n_head * width + n_head * nope * latent + n_head * span * (2 * latent + width - nope)
                       + n_head * latent * value + n_head * value * hidden)
    return pl.pallas_call(
        functools.partial(attention_kernel, width ** -0.5, n_q, n_tok),
        out_shape=(out, out),
        grid_spec=grid_spec,
        cost_estimate=pl.CostEstimate(flops=flops, bytes_accessed=2 * cache.size, transcendentals=0),
        name='attention_layer',
    )(kv_lens, x, w_q.transpose(1, 2, 0).reshape(n_head * width, hidden), w_uk, *tables, cache.transpose(0, 2, 1),
      w_uv, w_o.reshape(n_head * value, hidden))


def xor_send(vals, mask):
    return lax.ppermute(vals, FLAT_AXES, [(dev, dev ^ mask) for dev in range(16)])


def gather_tp(rows):
    return [rows] + [xor_send(rows, 4 * rel) for rel in (1, 2, 3)]


def reduce_tp(lead_keep, lead_send, tail_keep, tail_send):
    tok = lead_keep.shape[0] // 2
    lead_in = xor_send(lead_send, 8)
    tail_in = xor_send(tail_send, 4)
    lead_far = xor_send(lead_keep[tok:] + lead_in[tok:], 4)
    tail_far = xor_send(tail_keep[tok:] + tail_in[tok:], 8)
    lead_own = lead_keep[:tok] + lead_in[:tok] + lead_far
    tail_own = tail_keep[:tok] + tail_in[:tok] + tail_far
    return jnp.concatenate([lead_own, tail_own], axis=-1)


def solution(mesh):
    n_dev = mesh.shape['tp'] * mesh.shape['ep']
    rows_spec = P(FLAT_AXES, None)
    cube_spec = P(FLAT_AXES, None, None)
    whole_spec = P(None, None, None)
    col_split = P(None, 'tp')
    row_split = P('tp', None)
    in_specs = (rows_spec, cube_spec, cube_spec, P(FLAT_AXES), rows_spec, rows_spec,
                whole_spec, whole_spec, whole_spec, whole_spec, whole_spec, whole_spec, whole_spec, whole_spec,
                col_split, col_split, row_split, col_split, col_split, row_split,
                cube_spec, cube_spec, cube_spec)

    def body(hidden_in, cache0, cache1, kv_lens, route_ids, route_wts, att0_q, att0_uk, att0_uv, att0_o, att1_q, att1_uk, att1_uv, att1_o, ffn0_gate, ffn0_up, ffn0_down, ffn1_gate, ffn1_up, ffn1_down, exp_gate, exp_up, exp_down):
        tok, top_k = route_ids.shape
        cap = min(tok, (2 * tok * top_k + n_dev - 1) // n_dev)
        pos, gpos, gwt = route_tables(route_ids.T, route_wts.T, cap)
        hidden_in, pos = lax.optimization_barrier((hidden_in, pos))
        zero_wt = jnp.sum(jnp.where(route_ids >= n_dev, route_wts, 0.0), axis=1, keepdims=True)
        tables = rotary_tables(kv_lens, att0_q.shape[2] - att0_uk.shape[1], 4)

        h_zero, u_zero = attention(hidden_in, cache0, kv_lens, tables, att0_q, att0_uk, att0_uv, att0_o)
        grp = gather_tp(u_zero)
        far = []
        for rel in range(4):
            far.append(xor_send(grp[rel], 2))
        near = []
        for rel in range(4):
            near.append(xor_send(grp[rel], 1))
        cross = [xor_send(rows, 1) for rows in far]
        part0 = dense_partial(grp, ffn0_gate, ffn0_up, ffn0_down)
        blocks = [rows for rel in range(4) for rows in (grp[rel], near[rel], far[rel], cross[rel])]
        pos, part0 = lax.optimization_barrier((pos, part0))
        exp_out = expert_rows(pos, blocks, exp_gate[0], exp_up[0], exp_down[0], cap)
        back = [exp_out[0]] + [xor_send(exp_out[off], off) for off in (1, 2, 3)]

        f_zero = (h_zero.astype(jnp.float32) + reduce_tp(*part0)).astype(jnp.bfloat16)
        h_one, u_one = attention(f_zero, cache1, kv_lens, tables, att1_q, att1_uk, att1_uv, att1_o)
        grp1 = gather_tp(u_one)
        mix = mix_rows(gpos, gwt, back, tok, cap)
        part1 = dense_partial(grp1, ffn1_gate, ffn1_up, ffn1_down, mix)
        total = reduce_tp(*part1)
        return (h_one.astype(jnp.float32) + zero_wt * u_zero.astype(jnp.float32) + total).astype(jnp.bfloat16)

    return jax.shard_map(body, mesh=mesh, in_specs=in_specs, out_specs=rows_spec, check_vma=False)
```
